32 devices in a mesh: hist: 4 (over z), rows: 2 (over y), dom: 4 (over x, core).
Axes of the slice: x: 2, y: 2, z: 4, core: 2. Of those that a mesh axis runs over, the one named last changes fastest.
Arguments:
- row_index: int32 [4, 32768], P(None, ('hist', 'rows', 'dom')), may hold values from 0 to 510
- col_index: int32 [4, 32768], P(None, ('hist', 'rows', 'dom')), may hold values from 0 to 510
- bin_index: int32 [4, 32768], P(None, ('hist', 'rows', 'dom')), may hold values from 0 to 255
- charge: bfloat16 [32768], P(('hist', 'rows', 'dom')), may hold values from 0.5 to 2
- momentum: float32 [2, 32768], P(None, ('hist', 'rows', 'dom')), may hold values from -6 to 6
- history: bfloat16 [32, 512, 512], P('hist', 'rows'), may hold values from 0 to 2
- kernel_cols: bfloat16 [32, 512, 512], P('hist', 'dom'), may hold values from -0.25 to 0.25
- kernel_rows: bfloat16 [32, 512, 2, 512], P('hist', 'rows'), may hold values from -0.046875 to 0.046875
Outputs:
- momentum_out: float32 [2, 32768], P(None, ('hist', 'rows', 'dom'))
- history_out: bfloat16 [32, 512, 512], P('hist', 'rows')
The draws below stay inside these ranges and needn't reach their ends.
All inputs are finite; a program needn't handle non-finite values.
Results may differ from the reference program's by a relative error of at most 0.0024.
Values may be sent and summed in bfloat16 or wider, within the bound.
A program may use at most 64 MiB of HBM per device.

```python
import math
import jax
import jax.numpy as jnp
from jax import lax

NG = 512
BINS = 16
STEPS = 4
LAGS = 32
PARTICLES = 32768


def draw_row_index(key, part):
    shuffled = jax.random.permutation(jax.random.fold_in(key, 7), PARTICLES).astype(jnp.int32)
    centre = shuffled * (NG - 1) // PARTICLES
    drift_rows = jnp.arange(STEPS, dtype=jnp.int32)[:, None] - STEPS // 2
    jitter = jax.random.randint(jax.random.fold_in(key, 11), (STEPS, PARTICLES), -4, 5, dtype=jnp.int32)
    return jnp.clip(centre[None, :] + drift_rows + jitter, 0, NG - 2).astype(jnp.int32)


def set_ends(result, rng, smallest, high):
    extent = result.shape
    index_at = [jax.random.randint(jax.random.fold_in(rng, axis), (), 0, extent[axis]) for axis in range(len(extent))]
    result = result.at[tuple(index_at)].set(smallest)
    longest = extent.index(max(extent))
    index_at[longest] = (index_at[longest] + 1) % extent[longest]
    return result.at[tuple(index_at)].set(high)


def levels(key, dims, pieces, low, high):
    loudness, own = 1.0, jax.random.fold_in(key, 6)
    for position, blocks in pieces:
        draws = jnp.exp(jax.random.uniform(jax.random.fold_in(own, position), (blocks,), jnp.float32, low / len(pieces), high / len(pieces)))
        loudness = loudness * jnp.repeat(draws, dims[position] // blocks).reshape([-1 if axis == position else 1 for axis in range(len(dims))])
    return loudness


def noise(key, extent, deviation, limit, pieces=(), kind=jnp.bfloat16):
    drawn = jax.random.normal(key, extent, jnp.float32) * deviation
    if len(pieces) > 0:
        drawn = levels(key, extent, pieces, -0.22, 0.18) * drawn
    return jnp.clip(drawn, min=-limit, max=limit).astype(kind)


def setup_inputs(seed: int = 0) -> dict:
    arg_keys = jax.random.split(jax.random.key(seed), 9)
    row_index = draw_row_index(jax.random.fold_in(arg_keys[8], 71), 0)
    col_index = set_ends(jax.random.randint(arg_keys[1], (STEPS, PARTICLES), 0, NG - 1), jax.random.fold_in(arg_keys[1], 1), 0, (NG - 1) - 1).astype(jnp.int32)
    bin_index = set_ends(jax.random.randint(arg_keys[2], (STEPS, PARTICLES), 0, BINS * BINS), jax.random.fold_in(arg_keys[2], 1), 0, (BINS * BINS) - 1).astype(jnp.int32)
    charge = jnp.clip(jnp.exp(math.log(2.0) - 1.3862944 * jax.random.uniform(arg_keys[3], (PARTICLES,), jnp.float32) ** levels(arg_keys[3], (PARTICLES,), ((0, 32),), -0.2, 0.2)), 0.5, 2.0).astype(jnp.bfloat16)
    momentum = noise(arg_keys[4], (2, PARTICLES), 1.0, 6.0, ((1, 32),), jnp.float32)
    history = jnp.clip(2.0 * jax.random.uniform(arg_keys[5], (LAGS, NG, NG), jnp.float32) ** levels(arg_keys[5], (LAGS, NG, NG), ((0, 4), (1, 2)), -0.2, 0.2), 0.0, 2.0).astype(jnp.bfloat16)
    kernel_cols = noise(arg_keys[6], (LAGS, NG, NG), NG ** -0.5, 0.25, ((0, 4), (1, 4)))
    kernel_rows = noise(arg_keys[7], (LAGS, NG, 2, NG), (NG * LAGS) ** -0.5, 0.046875, ((0, 4), (1, 2)))
    return {"row_index": row_index, "col_index": col_index, "bin_index": bin_index, "charge": charge, "momentum": momentum, "history": history, "kernel_cols": kernel_cols, "kernel_rows": kernel_rows}


kick_scale = 0.5


def rounded(values):
    return lax.optimization_barrier(values.astype(jnp.bfloat16)).astype(jnp.float32)


def reference(row_index, col_index, bin_index, charge, momentum, history, kernel_cols, kernel_rows):
    charge_f = charge.astype(jnp.float32)
    cols_wide = kernel_cols.astype(jnp.float32)
    rows_wide = kernel_rows.astype(jnp.float32)
    cycle_now = history
    kick_sum = jnp.zeros((PARTICLES, 2), jnp.float32)
    for turn_index in range(STEPS):
        row_now = row_index[turn_index].astype(jnp.int32)
        col_now = col_index[turn_index].astype(jnp.int32)
        bin_now = bin_index[turn_index]
        frac_row = ((bin_now // BINS).astype(jnp.float32) + 0.5) / BINS
        frac_col = ((bin_now % BINS).astype(jnp.float32) + 0.5) / BINS
        lower = rounded(charge_f * (1.0 - frac_row))
        upper = rounded(charge_f * frac_row)
        density = jnp.zeros((NG, NG), jnp.float32)
        density = density.at[row_now, col_now].add(lower * (1.0 - frac_col))
        density = density.at[row_now, col_now + 1].add(lower * frac_col)
        density = density.at[row_now + 1, col_now].add(upper * (1.0 - frac_col))
        density = density.at[row_now + 1, col_now + 1].add(upper * frac_col)
        newest = density.astype(jnp.bfloat16)
        cycle_now = jnp.concatenate([newest[None], cycle_now[:-1]], axis=0)
        mixed_rows = jnp.einsum("kab,kjb->kaj", cycle_now.astype(jnp.float32), cols_wide).astype(jnp.bfloat16)
        field_full = rounded(jnp.einsum("kaci,kaj->icj", rows_wide, mixed_rows.astype(jnp.float32)))
        corner_aa = field_full[row_now, :, col_now]
        corner_ba = field_full[row_now + 1, :, col_now]
        corner_ab = field_full[row_now, :, col_now + 1]
        corner_bb = field_full[row_now + 1, :, col_now + 1]
        weight_row = frac_row[:, None]
        weight_col = frac_col[:, None]
        near_col = (1.0 - weight_row) * corner_aa + weight_row * corner_ba
        far_col = (1.0 - weight_row) * corner_ab + weight_row * corner_bb
        kick_sum = kick_sum + ((1.0 - weight_col) * near_col + weight_col * far_col)
    momentum_out = momentum + kick_scale * kick_sum.T
    return momentum_out, cycle_now
```

```python
import functools
import jax
import jax.numpy as jnp
from jax import lax
from jax.experimental import pallas as pl
from jax.experimental.pallas import tpu as pltpu
from jax.sharding import PartitionSpec as P

NG = 512
BINS = 16
STEPS = 4
CORES = 2
HALVES = 4
kick_scale = 0.5

MESH = pl.DeviceIdType.MESH
VM = pl.BlockSpec(memory_space=pltpu.VMEM)
NT = (((1,), (1,)), ((), ()))


def place():
    return lax.axis_index("hist"), lax.axis_index("rows"), lax.axis_index("dom")


def hat(extent, whole, near, far):
    kind = jnp.bfloat16
    places = lax.broadcasted_iota(jnp.int32, (extent, whole.shape[1]), 0).astype(kind)
    first = whole.astype(kind)
    return jnp.where(places == first, near.astype(kind),
                     jnp.where(places == first + kind(1.0), far.astype(kind), kind(0.0)))


def plane_peer(rows, dom, shift):
    h, r, d = place()
    other = lax.rem(r * dom + d + shift, rows * dom)
    return other, (h, other // dom, lax.rem(other, dom))


def inside(index, count):
    return jnp.logical_and(index >= 0, index < count)


def kernel(hist, rows, dom, row_ref, col_ref, bin_ref, charge_ref, momentum, old_ref, cols_ref, rows_ref,
           out, newest, spots, base, frac, dens, summed, arrived, gath, grids, cols, raw, turned, total,
           parts, got, mine, from_low, from_high, to_high, to_low, kicks, got_kicks, load,
           sem_as, sem_ar, sem_hs, sem_hr, sem_cs, sem_cr, sem_xs, sem_xr, sem_ps, sem_pr, sem_fs, sem_fr,
           sem_ys, sem_yr, sem_us, sem_ur, sem_ds, sem_dr, sem_ks, sem_kr):
    h, r, d = place()
    n = rows * dom
    lags, width, _ = cols.shape
    band = old_ref.shape[1]
    piece = NG // rows
    size = width // HALVES
    kind = parts.dtype
    chips = dom // CORES
    up, down = (h + 1, r, d), (h - 1, r, d)
    levels = (hist - 1).bit_length()
    sums = [jnp.logical_and(lax.rem(h, 2 << a) == 0, h + (1 << a) < hist) for a in range(levels)]
    gives = [lax.rem(h, 2 << a) == 1 << a for a in range(levels)]
    rank = sum(jnp.where(lax.rem(h, 1 << a) == 0, 1, 0) for a in range(1, levels + 1))
    partner = (h, r, d + 1 - 2 * lax.rem(d, CORES))
    across = [(h, r, lax.rem(d + CORES * j, dom)) for j in range(1, chips)]
    is_first, is_last = h == 0, h == hist - 1
    below, above = jnp.logical_not(is_last), jnp.logical_not(is_first)
    inner = jnp.logical_and(below, above)

    loads = (pltpu.make_async_copy(old_ref, grids.at[pl.ds(STEPS, lags)], load.at[0]),
             pltpu.make_async_copy(cols_ref, cols, load.at[1]),
             pltpu.make_async_copy(rows_ref, raw, load.at[2]))
    for copy in loads:
        copy.start()
    barrier = pltpu.get_barrier_semaphore()

    @pl.when(below)
    def _():
        pl.semaphore_signal(barrier, inc=1, device_id=up, device_id_type=MESH)

    @pl.when(above)
    def _():
        pl.semaphore_signal(barrier, inc=1, device_id=down, device_id_type=MESH)

    for shift in range(1, n):
        pl.semaphore_signal(barrier, inc=1, device_id=plane_peer(rows, dom, shift)[1], device_id_type=MESH)
    count = n - 1 + jnp.where(is_first, 0, 1) + jnp.where(is_last, 0, 1)
    for a in range(1, levels):
        count += jnp.where(jnp.logical_or(sums[a], gives[a]), 1, 0)

        @pl.when(sums[a])
        def _():
            pl.semaphore_signal(barrier, inc=1, device_id=(h + (1 << a), r, d), device_id_type=MESH)

        @pl.when(gives[a])
        def _():
            pl.semaphore_signal(barrier, inc=1, device_id=(h - (1 << a), r, d), device_id_type=MESH)

    bins = bin_ref[...]
    row_bin = bins // BINS
    spots[0, 0:STEPS] = row_ref[...].astype(jnp.float32) + (row_bin.astype(jnp.float32) + 0.5) / BINS
    spots[0, STEPS:2 * STEPS] = (col_ref[...].astype(jnp.float32)
                                 + ((bins - row_bin * BINS).astype(jnp.float32) + 0.5) / BINS)
    spots[0, 2 * STEPS:] = charge_ref[...].astype(jnp.float32).reshape(1, -1)
    pl.semaphore_wait(barrier, count)

    def remote(src, dst, s_sem, r_sem, device):
        return pltpu.make_async_remote_copy(src_ref=src, dst_ref=dst, send_sem=s_sem, recv_sem=r_sem,
                                            device_id=device, device_id_type=MESH)

    def spot_copy(shift):
        return remote(spots.at[0], spots.at[shift], sem_as.at[shift], sem_ar.at[shift],
                      plane_peer(rows, dom, shift)[1])

    def tail_copy(s):
        columns = pl.ds(pl.multiple_of(d * width, width), width)
        return remote(old_ref.at[lags - 1 - s, :, columns], gath.at[d, s], sem_hs.at[s], sem_hr.at[s], up)

    def tree_copy(s, a):
        return remote(summed.at[s], arrived.at[s, a], sem_cs.at[s, a], sem_cr.at[s, a], (h - (1 << a), r, d))

    def cross_copy(s, j):
        return remote(gath.at[d, s], gath.at[d, s], sem_xs.at[s, j], sem_xr.at[s, j], across[j - 1])

    def partner_copy(s):
        return remote(gath.at[d, s], gath.at[d, s], sem_ps.at[s], sem_pr.at[s], partner)

    def forward_copy(s, j):
        other = lax.rem(d + CORES * (chips - j), dom)
        return remote(gath.at[other, s], gath.at[other, s], sem_fs.at[s, j], sem_fr.at[s, j], partner)

    def span(c):
        return pl.ds(pl.multiple_of(c * size, size), size)

    def row_copy(c, j):
        other = lax.rem(r + j, rows)
        return remote(parts.at[other, span(c)], got.at[j, span(c)], sem_ys.at[c, j], sem_yr.at[c, j],
                      (h, other, d))

    def up_copy(c):
        return remote(to_high.at[span(c)], from_low.at[span(c)], sem_us.at[c], sem_ur.at[c], up)

    def down_copy(c):
        return remote(to_low.at[span(c)], from_high.at[span(c)], sem_ds.at[c], sem_dr.at[c], down)

    def kick_copy(k):
        return remote(kicks.at[k], got_kicks.at[k], sem_ks.at[k], sem_kr.at[k], plane_peer(rows, dom, n - k)[1])

    for shift in range(1, n):
        spot_copy(shift).start()

    @pl.when(below)
    def _():
        for s in range(STEPS):
            tail_copy(s).start()

    total[...] = jnp.zeros_like(total)
    dens[...] = jnp.zeros_like(dens)
    kicks[...] = jnp.zeros_like(kicks)
    for copy in loads:
        copy.wait()

    def add_field(weights, mixed, where):
        for comp in range(2):
            total[comp, where] += jnp.dot(mixed, weights[comp], preferred_element_type=jnp.float32)

    def products(k, weights, start, steps):
        window = grids[pl.ds(start, steps)].reshape(steps * band, NG)
        mixed = lax.dot_general(cols[k], window, NT, preferred_element_type=jnp.float32).astype(kind)
        stacked = jnp.concatenate(
            [mixed[:, (steps - 1 - s) * band:(steps - s) * band] for s in range(steps)], axis=0)
        add_field(weights, stacked, pl.ds(0, steps * width))

    def whole_lag(k):
        products(k, pltpu.einshape("acb->cab", raw[k]), k, STEPS)

    ahead = max(0, lags - STEPS - 2)

    def lag(k, carry):
        whole_lag(k)
        return carry

    lax.fori_loop(STEPS, STEPS + ahead, lag, 0)
    turned[0] = pltpu.einshape("acb->cab", raw[0])
    for k in range(1, STEPS):
        turned[k] = pltpu.einshape("acb->cab", raw[k])
        products(k, turned[k], STEPS, k)

    side = lax.broadcasted_iota(jnp.int32, (2 * STEPS, 1), 0)
    corner = jnp.where(side < STEPS, r * band, d * width).astype(jnp.float32)

    def settle(k):
        value = spots[k, 0:2 * STEPS]
        floor = jnp.floor(value)
        base[k] = floor - corner
        frac[k] = value - floor

    settle(0)

    def arrive(k, carry):
        spot_copy(k).wait_recv()
        settle(k)
        return carry

    lax.fori_loop(1, n, arrive, 0)

    def row_of(k, s):
        return base[k, pl.ds(s, 1), :], frac[k, pl.ds(s, 1), :]

    def deposit(s):
        def block(k, carry):
            charge = spots[k, 2 * STEPS:, :]
            row, up_row = row_of(k, s)
            col, up_col = row_of(k, STEPS + s)
            left = hat(band, row, charge * (1.0 - up_row), charge * up_row)
            right = hat(width, col, 1.0 - up_col, up_col)
            dens[s] += lax.dot_general(left, right, NT, preferred_element_type=jnp.float32)
            return carry

        lax.fori_loop(0, n, block, 0, unroll=4)

    def relay(s):
        for a in range(levels):
            @pl.when(sums[a])
            def _():
                tree_copy(s, a).wait_recv()
                dens[s] += arrived[s, a].astype(jnp.float32)

        @pl.when(is_first)
        def _():
            gath[d, s] = dens[s].astype(kind)

        @pl.when(above)
        def _():
            summed[s] = dens[s].astype(kind)

        for a in range(levels):
            @pl.when(gives[a])
            def _():
                tree_copy(s, a).start()

    def gather(s):
        @pl.when(above)
        def _():
            tail_copy(s).wait_recv()

        for j in range(1, chips):
            cross_copy(s, j).start()
        partner_copy(s).start()

    def forward(s):
        for j in range(1, chips):
            cross_copy(s, j).wait_recv()
            forward_copy(s, j).start()

    def late(s):
        partner_copy(s).wait_recv()
        for j in range(1, chips):
            forward_copy(s, j).wait_recv()
        grid = jnp.concatenate([gath[e, s] for e in range(dom)], axis=1)
        grids[STEPS - 1 - s] = grid
        newest[STEPS - 1 - s] = grid
        where = pl.ds(pl.multiple_of(s * width, width), width)

        def add(k, carry):
            mixed = lax.dot_general(cols[k], grids[STEPS - 1 - s + k], NT,
                                    preferred_element_type=jnp.float32).astype(kind)
            add_field(turned[k], mixed, where)
            return carry

        lax.fori_loop(0, s + 1, add, 0)
        for q in range(rows):
            block = jnp.concatenate([total[comp, where, q * piece:(q + 1) * piece] for comp in range(2)], axis=1)

            @pl.when(r == q)
            def _():
                mine[where] = block

            @pl.when(r != q)
            def _():
                parts[q, where] = block.astype(kind)

        for half in range(HALVES):
            for j in range(1, rows):
                row_copy(s * HALVES + half, j).start()

    def spread(s):
        for half in range(HALVES):
            c = s * HALVES + half
            value = mine[span(c)]
            for j in range(1, rows):
                row_copy(c, j).wait_recv()
                value += got[j, span(c)].astype(jnp.float32)
            mine[span(c)] = value

            @pl.when(is_first)
            def _():
                to_high[span(c)] = value.astype(kind)
                up_copy(c).start()

            @pl.when(is_last)
            def _():
                to_low[span(c)] = value.astype(kind)
                down_copy(c).start()

    def rise(s):
        for half in range(HALVES):
            c = s * HALVES + half
            up_copy(c).wait_recv()

            @pl.when(inner)
            def _():
                to_high[span(c)] = (mine[span(c)] + from_low[span(c)].astype(jnp.float32)).astype(kind)
                up_copy(c).start()

    def sink(s):
        for half in range(HALVES):
            c = s * HALVES + half
            down_copy(c).wait_recv()

            @pl.when(inner)
            def _():
                to_low[span(c)] = (mine[span(c)] + from_high[span(c)].astype(jnp.float32)).astype(kind)
                down_copy(c).start()

    def kick(s):
        where = pl.ds(pl.multiple_of(s * width, width), width)

        @pl.when(above)
        def _():
            mine[where] = mine[where] + from_low[where].astype(jnp.float32)

        @pl.when(below)
        def _():
            mine[where] = mine[where] + from_high[where].astype(jnp.float32)

        value = mine[where]
        table = jnp.concatenate([value[:, :band], value[:, band:]], axis=0).astype(kind)

        def block(k, carry):
            row, up_row = row_of(k, s)
            col, up_col = row_of(k, STEPS + s)
            left = hat(band, row, 1.0 - up_row, up_row)
            right = hat(width, col, 1.0 - up_col, up_col).astype(jnp.float32)
            along = jnp.dot(table, left, preferred_element_type=jnp.float32)
            for comp in range(2):
                kicks[k, comp:comp + 1, :] += jnp.sum(
                    along[comp * width:(comp + 1) * width] * right, axis=0, keepdims=True)
            return carry

        lax.fori_loop(0, n, block, 0, unroll=2)

    early, level = STEPS + 1, 2 * levels
    row_off = jnp.where(is_first, level + 4, early + 4)
    rise_off, sink_off = early + 6 + h, early + 5 + (hist - 1 - h)
    kick_off = jnp.maximum(rise_off, sink_off) + jnp.where(is_first, 0, 2 * (hist - 1 - h))

    def at(index, action):
        @pl.when(inside(index, STEPS))
        def _():
            action(index)

    def tick(t, carry):
        at(t, deposit)
        at(t - 2 * rank, relay)
        ready = jnp.where(is_first, t - level, t)
        at(ready, gather)
        at(t - row_off, spread)

        @pl.when(above)
        def _():
            at(t - rise_off, rise)

        @pl.when(below)
        def _():
            at(t - sink_off, sink)

        at(jnp.where(is_first, t - level - 2, t - early), late)
        at(ready - 1, forward)
        spare = t - (STEPS - 1) + STEPS + ahead

        @pl.when(jnp.logical_and(t >= STEPS - 1, spare < lags))
        def _():
            whole_lag(spare)

        at(t - kick_off, kick)
        return carry

    lax.fori_loop(0, STEPS + max(early + 5 + hist - 1, early + 6 + hist - 1, early + 5 + 3 * (hist - 2)
                                 + 1, early + 5 + hist), tick, 0)

    for k in range(1, n):
        kick_copy(k).start()
    for shift in range(1, n):
        spot_copy(shift).wait_send()
    for s in range(STEPS):
        partner_copy(s).wait_send()
        for j in range(1, chips):
            forward_copy(s, j).wait_send()
            cross_copy(s, j).wait_send()

    @pl.when(above)
    def _():
        for c in range(STEPS * HALVES):
            down_copy(c).wait_send()

    for a in range(levels):
        @pl.when(gives[a])
        def _():
            for s in range(STEPS):
                tree_copy(s, a).wait_send()

    @pl.when(below)
    def _():
        for s in range(STEPS):
            tail_copy(s).wait_send()
        for c in range(STEPS * HALVES):
            up_copy(c).wait_send()

    for c in range(STEPS * HALVES):
        for j in range(1, rows):
            row_copy(c, j).wait_send()
    sum_all = kicks[0]
    for k in range(1, n):
        kick_copy(k).wait()
        sum_all = sum_all + got_kicks[k]
    out[...] = momentum[...] + kick_scale * sum_all


def local(hist, rows, dom, row_index, col_index, bin_index, charge, momentum, history, kernel_cols, kernel_rows):
    lags, band, _ = history.shape
    width = kernel_cols.shape[1]
    own = row_index.shape[1]
    n = rows * dom
    chips, levels = dom // CORES, (hist - 1).bit_length()
    tall, wide = STEPS * width, 2 * NG // rows
    count = STEPS * HALVES
    kind, wider = jnp.bfloat16, jnp.float32
    dma, vmem = pltpu.SemaphoreType.DMA, pltpu.VMEM
    anywhere = pl.BlockSpec(memory_space=pl.ANY)
    tile = (STEPS, band, width)
    flat = vmem((tall, wide), kind)
    each = vmem((n,) + momentum.shape, wider)
    moved, newest = pl.pallas_call(
        functools.partial(kernel, hist, rows, dom),
        out_shape=(jax.ShapeDtypeStruct(momentum.shape, wider),
                   jax.ShapeDtypeStruct((STEPS, band, NG), kind)),
        in_specs=[VM] * 5 + [anywhere] * 3, out_specs=(VM, VM),
        scratch_shapes=[vmem((n, 2 * STEPS + 1, own), wider), vmem((n, 2 * STEPS, own), wider),
                        vmem((n, 2 * STEPS, own), wider), vmem(tile, wider), vmem(tile, kind), vmem((STEPS, levels) + tile[1:], kind),
                        vmem((dom,) + tile, kind), vmem((lags + STEPS, band, NG), kind),
                        vmem(kernel_cols.shape, kind), vmem(kernel_rows.shape, kind),
                        vmem((STEPS, 2, band, NG), kind), vmem((2, tall, NG), wider),
                        vmem((rows, tall, wide), kind), vmem((rows, tall, wide), kind), vmem((tall, wide), wider),
                        flat, flat, flat, flat, each, each, dma((3,)), dma((n,)), dma((n,))]
        + [dma((STEPS,))] * 2 + [dma((STEPS, levels))] * 2 + [dma((STEPS, chips))] * 2 + [dma((STEPS,))] * 2 + [dma((STEPS, chips))] * 2
        + [dma((count, rows))] * 2 + [dma((count,))] * 4 + [dma((n,))] * 2,
        compiler_params=pltpu.CompilerParams(collective_id=1, has_side_effects=True),
    )(row_index, col_index, bin_index, charge, momentum, history, kernel_cols, kernel_rows)
    return moved, jnp.concatenate([newest, history[:-STEPS]], axis=0)


def solution(mesh):
    spread = ("hist", "rows", "dom")
    in_specs = (P(None, spread), P(None, spread), P(None, spread), P(spread), P(None, spread),
                P("hist", "rows", None), P("hist", "dom", None), P("hist", "rows", None, None))
    out_specs = (P(None, spread), P("hist", "rows", None))
    sizes = mesh.shape
    body = functools.partial(local, sizes["hist"], sizes["rows"], sizes["dom"])
    return jax.shard_map(body, mesh=mesh, in_specs=in_specs, out_specs=out_specs, check_vma=False)
```

```python
import functools
import jax
import jax.numpy as jnp
from jax import lax
from jax.experimental import pallas as pl
from jax.experimental.pallas import tpu as pltpu
from jax.sharding import PartitionSpec as P

NG = 512
BINS = 16
STEPS = 4
CORES = 2
HALVES = 4
kick_scale = 0.5

MESH = pl.DeviceIdType.MESH
VM = pl.BlockSpec(memory_space=pltpu.VMEM)
NT = (((1,), (1,)), ((), ()))


def place():
    return lax.axis_index("hist"), lax.axis_index("rows"), lax.axis_index("dom")


def hat(extent, whole, near, far):
    kind = jnp.bfloat16
    places = lax.broadcasted_iota(jnp.int32, (extent, whole.shape[1]), 0).astype(kind)
    first = whole.astype(kind)
    return jnp.where(places == first, near.astype(kind),
                     jnp.where(places == first + kind(1.0), far.astype(kind), kind(0.0)))


def plane_peer(rows, dom, shift):
    h, r, d = place()
    other = lax.rem(r * dom + d + shift, rows * dom)
    return other, (h, other // dom, lax.rem(other, dom))


def drain(ref, sem):
    pltpu.make_async_copy(ref, ref, sem).wait()


def inside(index, count):
    return jnp.logical_and(index >= 0, index < count)


def kernel(hist, rows, dom, row_ref, col_ref, bin_ref, charge_ref, momentum, old_ref, cols_ref, rows_ref,
           out, newest, places, charge_in, start, spots, charges, base, frac, lefts, rights, dens, summed, arrived, gath, grids, cols, raw, turned, total,
           parts, got, mine, from_low, from_high, to_high, to_low, table, kicks, got_kicks, load, sent, once,
           sem_a, sem_h, sem_c, sem_x, sem_g, sem_y, sem_u, sem_d):
    h, r, d = place()
    n = rows * dom
    lags, width, _ = cols.shape
    band = old_ref.shape[1]
    keep = lefts.shape[0] == n
    piece = NG // rows
    size = width // HALVES
    kind = parts.dtype
    chips = dom // CORES
    up, down = (h + 1, r, d), (h - 1, r, d)
    levels = (hist - 1).bit_length()
    sums = [jnp.logical_and(lax.rem(h, 2 << a) == 0, h + (1 << a) < hist) for a in range(levels)]
    gives = [lax.rem(h, 2 << a) == 1 << a for a in range(levels)]
    rank = sum(jnp.where(lax.rem(h, 1 << a) == 0, 1, 0) for a in range(1, levels + 1))
    partner = (h, r, d + 1 - 2 * lax.rem(d, CORES))
    across = [(h, r, lax.rem(d + CORES * j, dom)) for j in range(1, chips)]
    is_first, is_last = h == 0, h == hist - 1
    below, above = jnp.logical_not(is_last), jnp.logical_not(is_first)
    inner = jnp.logical_and(below, above)

    loads = (pltpu.make_async_copy(old_ref, grids.at[pl.ds(STEPS, lags)], load.at[0]),
             pltpu.make_async_copy(cols_ref, cols, load.at[1]),
             pltpu.make_async_copy(rows_ref, raw, load.at[2]))
    small = [pltpu.make_async_copy(src, places.at[i], load.at[3])
             for i, src in enumerate((row_ref, col_ref, bin_ref))]
    small += [pltpu.make_async_copy(charge_ref, charge_in, load.at[4]),
              pltpu.make_async_copy(momentum, start, load.at[5])]
    for copy in small:
        copy.start()
    barrier = pltpu.get_barrier_semaphore()

    @pl.when(below)
    def _():
        pl.semaphore_signal(barrier, inc=1, device_id=up, device_id_type=MESH)

    @pl.when(above)
    def _():
        pl.semaphore_signal(barrier, inc=1, device_id=down, device_id_type=MESH)

    for shift in range(1, n):
        pl.semaphore_signal(barrier, inc=1, device_id=plane_peer(rows, dom, shift)[1], device_id_type=MESH)
    count = n - 1 + jnp.where(is_first, 0, 1) + jnp.where(is_last, 0, 1)
    for a in range(1, levels):
        count += jnp.where(jnp.logical_or(sums[a], gives[a]), 1, 0)

        @pl.when(sums[a])
        def _():
            pl.semaphore_signal(barrier, inc=1, device_id=(h + (1 << a), r, d), device_id_type=MESH)

        @pl.when(gives[a])
        def _():
            pl.semaphore_signal(barrier, inc=1, device_id=(h - (1 << a), r, d), device_id_type=MESH)

    for copy in loads:
        copy.start()
    drain(places, load.at[3])
    for copy in small[3:]:
        copy.wait()
    bins = places[2]
    row_bin = bins // BINS
    down_at = places[0].astype(jnp.float32) + (row_bin.astype(jnp.float32) + 0.5) / BINS
    over_at = places[1].astype(jnp.float32) + ((bins - row_bin * BINS).astype(jnp.float32) + 0.5) / BINS
    for s in range(STEPS):
        spots[0, s, 0:1, :] = down_at[s:s + 1]
        spots[0, s, 1:2, :] = over_at[s:s + 1]
    charges[0] = charge_in[...].astype(jnp.float32).reshape(1, -1)
    pl.semaphore_wait(barrier, count)

    def remote(src, dst, s_sem, r_sem, device):
        return pltpu.make_async_remote_copy(src_ref=src, dst_ref=dst, send_sem=s_sem, recv_sem=r_sem,
                                            device_id=device, device_id_type=MESH)

    def spot_copy(shift, s):
        return remote(spots.at[0, s], spots.at[shift, s], sent.at[0], sem_a.at[s],
                      plane_peer(rows, dom, shift)[1])

    def charge_copy(shift):
        return remote(charges.at[0], charges.at[shift], sent.at[1], once.at[0], plane_peer(rows, dom, shift)[1])

    def tail_copy(s):
        columns = pl.ds(pl.multiple_of(d * width, width), width)
        return remote(old_ref.at[lags - 1 - s, :, columns], gath.at[d, s], sent.at[2], sem_h.at[s], up)

    def tree_copy(s, a):
        return remote(summed.at[s], arrived.at[s, a], sent.at[3], sem_c.at[s, a], (h - (1 << a), r, d))

    def cross_copy(s, j):
        return remote(gath.at[d, s], gath.at[d, s], sent.at[4], sem_x.at[s, j - 1], across[j - 1])

    def partner_copy(s):
        return remote(gath.at[d, s], gath.at[d, s], sent.at[4], sem_g.at[s], partner)

    def forward_copy(s, j):
        other = lax.rem(d + CORES * (chips - j), dom)
        return remote(gath.at[other, s], gath.at[other, s], sent.at[4], sem_g.at[s], partner)

    def span(c):
        return pl.ds(pl.multiple_of(c * size, size), size)

    def row_copy(c, j):
        other = lax.rem(r + j, rows)
        return remote(parts.at[other, span(c)], got.at[j - 1, span(c)], sent.at[5], sem_y.at[c, j - 1],
                      (h, other, d))

    def up_copy(c):
        return remote(to_high.at[span(c)], from_low.at[span(c)], sent.at[6], sem_u.at[c], up)

    def down_copy(c):
        return remote(to_low.at[span(c)], from_high.at[span(c)], sent.at[7], sem_d.at[c], down)

    def kick_copy(k):
        return remote(kicks.at[k], got_kicks.at[k], sent.at[8], once.at[1], plane_peer(rows, dom, n - k)[1])

    def fresh(s):
        return pltpu.make_async_copy(grids.at[STEPS - 1 - s], newest.at[STEPS - 1 - s], load.at[6])

    for s in range(STEPS):
        for shift in range(1, n):
            spot_copy(shift, s).start()
            if s == 0:
                charge_copy(shift).start()

    @pl.when(below)
    def _():
        for s in range(STEPS):
            tail_copy(s).start()

    total[...] = jnp.zeros_like(total)
    dens[...] = jnp.zeros_like(dens)
    kicks[...] = jnp.zeros_like(kicks)
    for copy in loads:
        copy.wait()

    def add_field(weights, mixed, where):
        for comp in range(2):
            total[comp, where] += jnp.dot(mixed, weights[comp], preferred_element_type=jnp.float32)

    def products(k, weights, begin, steps, first=0):
        window = grids[pl.ds(begin, steps)].reshape(steps * band, NG)
        mixed = lax.dot_general(cols[k], window, NT, preferred_element_type=jnp.float32).astype(kind)
        stacked = jnp.concatenate(
            [mixed[:, (steps - 1 - s) * band:(steps - s) * band] for s in range(steps)], axis=0)
        add_field(weights, stacked, pl.ds(first * width, steps * width))

    def whole_lag(k):
        products(k, pltpu.einshape("acb->cab", raw[k]), k, STEPS)

    ahead = max(0, lags - STEPS - 2)

    def lag(k, carry):
        whole_lag(k)
        return carry

    lax.fori_loop(STEPS, STEPS + ahead, lag, 0)
    turned[0] = pltpu.einshape("acb->cab", raw[0])
    for k in range(1, STEPS):
        turned[k] = pltpu.einshape("acb->cab", raw[k])
        products(k, turned[k], STEPS, k)

    side = lax.broadcasted_iota(jnp.int32, (2, 1), 0)
    corner = jnp.where(side == 0, r * band, d * width).astype(jnp.float32)

    def settle(k, s):
        value = spots[k, s]
        floor = jnp.floor(value)
        base[k, s] = floor - corner
        frac[k, s] = value - floor

    def hats(k, s):
        whole, part = base[k, s], frac[k, s]
        left = hat(band, whole[0:1], 1.0 - part[0:1], part[0:1])
        right = hat(width, whole[1:2], 1.0 - part[1:2], part[1:2])
        return left, right

    def deposit(s):
        drain(spots.at[pl.ds(1, n - 1), s], sem_a.at[s])

        @pl.when(s == 0)
        def _():
            drain(charges.at[pl.ds(1, n - 1)], once.at[0])

        def arrive(k, carry):
            settle(k, s)
            return carry

        lax.fori_loop(0, n, arrive, 0, unroll=8)

        def block(k, carry):
            left, right = hats(k, s)
            if keep:
                lefts[k, s] = left
                rights[k, s] = right
            left = left * charges[k].astype(kind)
            dens[s] += lax.dot_general(left, right, NT, preferred_element_type=jnp.float32)
            return carry

        lax.fori_loop(0, n, block, 0, unroll=8)

    def relay(s):
        for a in range(levels):
            @pl.when(sums[a])
            def _():
                tree_copy(s, a).wait_recv()
                dens[s] += arrived[s, a].astype(jnp.float32)

        @pl.when(is_first)
        def _():
            gath[d, s] = dens[s].astype(kind)

        @pl.when(above)
        def _():
            summed[s] = dens[s].astype(kind)

        for a in range(levels):
            @pl.when(gives[a])
            def _():
                tree_copy(s, a).start()

    def gather(s):
        @pl.when(above)
        def _():
            tail_copy(s).wait_recv()

        for j in range(1, chips):
            cross_copy(s, j).start()
        partner_copy(s).start()

    def forward(s):
        for j in range(1, chips):
            cross_copy(s, j).wait_recv()
            forward_copy(s, j).start()

    def assemble(s):
        drain(gath.at[pl.ds(0, chips), s], sem_g.at[s])
        grids[STEPS - 1 - s] = jnp.concatenate([gath[e, s] for e in range(dom)], axis=1)
        fresh(s).start()

    def strip(s):
        return pl.ds(pl.multiple_of(s * width, width), width)

    def post(s):
        where = strip(s)
        for q in range(rows):
            block = jnp.concatenate([total[comp, where, q * piece:(q + 1) * piece] for comp in range(2)], axis=1)

            @pl.when(r == q)
            def _():
                mine[where] = block

            @pl.when(r != q)
            def _():
                parts[q, where] = block.astype(kind)

        for half in range(HALVES):
            for j in range(1, rows):
                row_copy(s * HALVES + half, j).start()

    def add_late(k, s):
        mixed = lax.dot_general(cols[k], grids[STEPS - 1 - s], NT, preferred_element_type=jnp.float32).astype(kind)
        add_field(turned[k], mixed, strip(s + k))

    def late(s):
        assemble(s)
        add_late(0, s)
        post(s)

    def late_more(s):
        def add(k, carry):
            add_late(k, s)
            return carry

        lax.fori_loop(1, STEPS - s, add, 0)

    def late_all(_):
        for s in range(STEPS):
            assemble(s)
        for k in range(STEPS):
            products(k, turned[k], k, STEPS - k, k)
        for s in range(STEPS):
            post(s)

    def spread(c):
        value = mine[span(c)]
        for j in range(1, rows):
            row_copy(c, j).wait_recv()
            value += got[j - 1, span(c)].astype(jnp.float32)
        mine[span(c)] = value

        @pl.when(is_first)
        def _():
            to_high[span(c)] = value.astype(kind)
            up_copy(c).start()

        @pl.when(is_last)
        def _():
            to_low[span(c)] = value.astype(kind)
            down_copy(c).start()

    def rise(c):
        up_copy(c).wait_recv()

        @pl.when(inner)
        def _():
            to_high[span(c)] = (mine[span(c)] + from_low[span(c)].astype(jnp.float32)).astype(kind)
            up_copy(c).start()

    def sink(c):
        down_copy(c).wait_recv()

        @pl.when(inner)
        def _():
            to_low[span(c)] = (mine[span(c)] + from_high[span(c)].astype(jnp.float32)).astype(kind)
            down_copy(c).start()

    def side_hat(k, s, c):
        tall = 2 * size
        whole, part = base[k, s], frac[k, s]
        shift = ((lax.rem(c, HALVES) // 2) * tall).astype(jnp.float32)
        return hat(tall, whole[1:2] - shift, 1.0 - part[1:2], part[1:2]).astype(jnp.float32)

    def kick(c):
        s, part = c // HALVES, lax.rem(c, 2)
        share, tall = n // 2, 2 * size
        rows_c = pl.ds(pl.multiple_of((c // 2) * tall, tall), tall)
        cols_c = pl.ds(pl.multiple_of((lax.rem(c, HALVES) // 2) * tall, tall), tall)

        @pl.when(part == 0)
        def _():
            value = mine[rows_c]
            value += jnp.where(above, from_low[rows_c].astype(jnp.float32), 0.0)
            value += jnp.where(below, from_high[rows_c].astype(jnp.float32), 0.0)
            table[0:tall] = value[:, :band].astype(kind)
            table[tall:] = value[:, band:].astype(kind)

        def block(i, carry):
            k = part * share + i
            left = lefts[k, s] if keep else hats(k, s)[0]
            right = rights[k, s, cols_c].astype(jnp.float32) if keep else side_hat(k, s, c)
            along = jnp.dot(table[...], left, preferred_element_type=jnp.float32)
            for comp in range(2):
                kicks[k, comp:comp + 1, :] += jnp.sum(
                    along[comp * tall:(comp + 1) * tall] * right, axis=0, keepdims=True)
            return carry

        lax.fori_loop(0, share, block, 0, unroll=4)

    early, level, pieces = STEPS + 1, 2 * levels, STEPS * HALVES
    begin, hop = HALVES * (early + 1), HALVES
    zero = HALVES * (level + 3) + HALVES // 2
    zero = HALVES * (level + 3) + 2
    row_lag = jnp.where(is_first, zero, begin)
    rise_lag = begin + 8 + 5 * (h - 1)
    sink_lag = jnp.where(is_first, zero + 12, begin + 4 + 4 * (hist - 2 - h))
    kick_lag = jnp.where(is_first, sink_lag, jnp.where(is_last, rise_lag, jnp.maximum(rise_lag, sink_lag))) + 1
    last = max(zero + 12, begin + 8 + 5 * (hist - 2), begin + max(8 + 5 * (hist - 3), 4 + 4 * (hist - 3))) + 1

    def at(index, action, count=STEPS):
        @pl.when(inside(index, count))
        def _():
            action(index)

    def tick(t, carry):
        at(t, deposit)

        @pl.when(is_first)
        def _():
            at(t - level - 2, late)

        at(t - 2 * rank, relay)
        at(jnp.where(is_first, t - level, 2 * t), gather)

        @pl.when(above)
        def _():
            at(2 * t + 1, gather)
            at(t - early, late_all, 1)

        def turn(i, carry):
            c = HALVES * t + i
            at(c - row_lag, spread, pieces)

            @pl.when(jnp.logical_and(below, sink_first))
            def _():
                at(c - sink_lag, sink, pieces)

            @pl.when(above)
            def _():
                at(c - rise_lag, rise, pieces)

            @pl.when(jnp.logical_not(sink_first))
            def _():
                at(c - sink_lag, sink, pieces)

            at(c - kick_lag, kick, pieces)
            return carry

        @pl.when(t >= min(early + 1, level + 3))
        def _():
            lax.fori_loop(0, HALVES, turn, 0)

        at(jnp.where(is_first, t - level - 1, 2 * (t - STEPS + 1)), forward)

        @pl.when(above)
        def _():
            at(2 * (t - STEPS + 1) + 1, forward)

        @pl.when(is_first)
        def _():
            at(t - level - 2, late_more)

        spare = STEPS + ahead + jnp.where(is_first, t - STEPS, t - STEPS + 1)

        @pl.when(jnp.logical_and(spare >= STEPS + ahead, spare < lags))
        def _():
            whole_lag(spare)

        return carry

    sink_first = h > 0
    lax.fori_loop(0, -(-(last + pieces) // HALVES), tick, 0)

    for k in range(1, n):
        kick_copy(k).start()
    drain(spots.at[pl.ds(0, n - 1)], sent.at[0])
    drain(charges.at[pl.ds(0, n - 1)], sent.at[1])
    drain(gath.at[pl.ds(0, 2 * chips - 1)], sent.at[4])
    drain(got, sent.at[5])
    pltpu.make_async_copy(grids.at[pl.ds(0, STEPS)], newest, load.at[6]).wait()

    @pl.when(above)
    def _():
        drain(summed, sent.at[3])
        drain(from_high, sent.at[7])

    @pl.when(below)
    def _():
        drain(gath.at[0], sent.at[2])
        drain(from_low, sent.at[6])

    drain(kicks.at[pl.ds(0, n - 1)], sent.at[8])
    drain(got_kicks.at[pl.ds(1, n - 1)], once.at[1])
    sum_all = kicks[0]
    for k in range(1, n):
        sum_all = sum_all + got_kicks[k]
    out[...] = start[...] + kick_scale * sum_all


def finish_kernel(moved, newest, old, out, history, writes):
    fresh, kept = newest.shape[0], history.shape[0] - newest.shape[0]
    stores = (pltpu.make_async_copy(newest, history.at[pl.ds(0, fresh)], writes.at[0]),
              pltpu.make_async_copy(old.at[pl.ds(0, kept)], history.at[pl.ds(fresh, kept)], writes.at[1]),
              pltpu.make_async_copy(moved, out, writes.at[2]))
    for copy in stores:
        copy.start()
    for copy in stores:
        copy.wait()


def finish(moved, newest, history):
    anywhere = pl.BlockSpec(memory_space=pl.ANY)
    return pl.pallas_call(
        finish_kernel,
        out_shape=(jax.ShapeDtypeStruct(moved.shape, moved.dtype), jax.ShapeDtypeStruct(history.shape, history.dtype)),
        in_specs=[VM] * 3, out_specs=(anywhere, anywhere),
        scratch_shapes=[pltpu.SemaphoreType.DMA((3,))],
        compiler_params=pltpu.CompilerParams(vmem_limit_bytes=8 * 2 ** 20),
    )(moved, newest, history)


def local(hist, rows, dom, row_index, col_index, bin_index, charge, momentum, history, kernel_cols, kernel_rows):
    lags, band, _ = history.shape
    width = kernel_cols.shape[1]
    own = row_index.shape[1]
    n = rows * dom
    chips, levels = dom // CORES, (hist - 1).bit_length()
    tall, wide = STEPS * width, 2 * NG // rows
    count = STEPS * HALVES
    kind, wider = jnp.bfloat16, jnp.float32
    dma, vmem = pltpu.SemaphoreType.DMA, pltpu.VMEM
    anywhere = pl.BlockSpec(memory_space=pl.ANY)
    tile = (STEPS, band, width)
    flat = vmem((tall, wide), kind)
    each = vmem((n,) + momentum.shape, wider)
    kept = n if n * STEPS * (band + width) * own * 2 <= 32 * 2 ** 20 else 1
    steps = (STEPS, own)
    spot = vmem((n, STEPS, 2, own), wider)
    moved, newest = pl.pallas_call(
        functools.partial(kernel, hist, rows, dom),
        out_shape=(jax.ShapeDtypeStruct(momentum.shape, wider),
                   jax.ShapeDtypeStruct((STEPS, band, NG), kind)),
        in_specs=[pl.BlockSpec(memory_space=pltpu.HBM)] * 8, out_specs=(VM, anywhere),
        scratch_shapes=[vmem((3,) + steps, jnp.int32), vmem((own,), kind),
                        vmem(momentum.shape, wider), spot, vmem((n, 1, own), wider), spot, spot,
                        vmem((kept, STEPS, band, own), kind), vmem((kept, STEPS, width, own), kind),
                        vmem(tile, wider), vmem(tile, kind), vmem((STEPS, levels) + tile[1:], kind),
                        vmem((dom,) + tile, kind), vmem((lags + STEPS, band, NG), kind),
                        vmem(kernel_cols.shape, kind), vmem(kernel_rows.shape, kind),
                        vmem((STEPS, 2, band, NG), kind), vmem((2, tall, NG), wider),
                        vmem((rows, tall, wide), kind), vmem((rows - 1, tall, wide), kind), vmem((tall, wide), wider),
                        flat, flat, flat, flat, vmem((4 * width // HALVES, band), kind), each, each, dma((7,)), dma((9,)), dma((2,)), dma((STEPS,)),
                        dma((STEPS,)), dma((STEPS, levels)), dma((STEPS, chips - 1)), dma((STEPS,)),
                        dma((count, rows - 1)), dma((count,)), dma((count,))],
        compiler_params=pltpu.CompilerParams(collective_id=1, has_side_effects=True,
                                             vmem_limit_bytes=50 * 2 ** 20),
    )(*(pltpu.with_memory_space_constraint(x, pltpu.HBM) for x in (
        row_index, col_index, bin_index, charge, momentum, history, kernel_cols, kernel_rows)))
    return finish(moved, newest, history)


def solution(mesh):
    spread = ("hist", "rows", "dom")
    in_specs = (P(None, spread), P(None, spread), P(None, spread), P(spread), P(None, spread),
                P("hist", "rows", None), P("hist", "dom", None), P("hist", "rows", None, None))
    out_specs = (P(None, spread), P("hist", "rows", None))
    sizes = mesh.shape
    body = functools.partial(local, sizes["hist"], sizes["rows"], sizes["dom"])
    return jax.shard_map(body, mesh=mesh, in_specs=in_specs, out_specs=out_specs, check_vma=False)
```

```python
import functools
import jax
import jax.numpy as jnp
from jax import lax
from jax.experimental import pallas as pl
from jax.experimental.pallas import tpu as pltpu
from jax.sharding import PartitionSpec as P

NG = 512
BINS = 16
STEPS = 4
CORES = 2
HALVES = 4
kick_scale = 0.5

MESH = pl.DeviceIdType.MESH
VM = pl.BlockSpec(memory_space=pltpu.VMEM)
NT = (((1,), (1,)), ((), ()))


def place():
    return lax.axis_index("hist"), lax.axis_index("rows"), lax.axis_index("dom")


def hat(extent, whole, near, far):
    kind = jnp.bfloat16
    places = lax.broadcasted_iota(jnp.int32, (extent, whole.shape[1]), 0).astype(kind)
    first = whole.astype(kind)
    return jnp.where(places == first, near.astype(kind),
                     jnp.where(places == first + kind(1.0), far.astype(kind), kind(0.0)))


def plane_peer(rows, dom, shift):
    h, r, d = place()
    other = lax.rem(r * dom + d + shift, rows * dom)
    return other, (h, other // dom, lax.rem(other, dom))


def drain(ref, sem):
    pltpu.make_async_copy(ref, ref, sem).wait()


def inside(index, count):
    return jnp.logical_and(index >= 0, index < count)


def kernel(hist, rows, dom, row_ref, col_ref, bin_ref, charge_ref, momentum, old_ref, cols_ref, rows_ref,
           out, newest, places, charge_in, start, spots, charges, base, frac, lefts, rights, dens, summed, arrived, gath, grids, cols, raw, turned, total,
           parts, got, mine, from_low, from_high, to_high, to_low, table, kicks, got_kicks, load, sent, once,
           sem_a, sem_h, sem_c, sem_x, sem_g, sem_y, sem_u, sem_d):
    h, r, d = place()
    n = rows * dom
    lags, width, _ = cols.shape
    band = old_ref.shape[1]
    keep = lefts.shape[0] == n
    piece = NG // rows
    size = width // HALVES
    kind = parts.dtype
    chips = dom // CORES
    up, down = (h + 1, r, d), (h - 1, r, d)
    levels = (hist - 1).bit_length()
    sums = [jnp.logical_and(lax.rem(h, 2 << a) == 0, h + (1 << a) < hist) for a in range(levels)]
    gives = [lax.rem(h, 2 << a) == 1 << a for a in range(levels)]
    rank = sum(jnp.where(lax.rem(h, 1 << a) == 0, 1, 0) for a in range(1, levels + 1))
    partner = (h, r, d + 1 - 2 * lax.rem(d, CORES))
    across = [(h, r, lax.rem(d + CORES * j, dom)) for j in range(1, chips)]
    is_first, is_last = h == 0, h == hist - 1
    below, above = jnp.logical_not(is_last), jnp.logical_not(is_first)
    inner = jnp.logical_and(below, above)

    loads = (pltpu.make_async_copy(old_ref, grids.at[pl.ds(STEPS, lags)], load.at[0]),
             pltpu.make_async_copy(cols_ref, cols, load.at[1]),
             pltpu.make_async_copy(rows_ref, raw, load.at[2]))
    small = [pltpu.make_async_copy(src, places.at[i], load.at[3])
             for i, src in enumerate((row_ref, col_ref, bin_ref))]
    small += [pltpu.make_async_copy(charge_ref, charge_in, load.at[4]),
              pltpu.make_async_copy(momentum, start, load.at[5])]
    for copy in small:
        copy.start()
    barrier = pltpu.get_barrier_semaphore()

    @pl.when(below)
    def _():
        pl.semaphore_signal(barrier, inc=1, device_id=up, device_id_type=MESH)

    @pl.when(above)
    def _():
        pl.semaphore_signal(barrier, inc=1, device_id=down, device_id_type=MESH)

    for shift in range(1, n):
        pl.semaphore_signal(barrier, inc=1, device_id=plane_peer(rows, dom, shift)[1], device_id_type=MESH)
    count = n - 1 + jnp.where(is_first, 0, 1) + jnp.where(is_last, 0, 1)
    for a in range(1, levels):
        count += jnp.where(jnp.logical_or(sums[a], gives[a]), 1, 0)

        @pl.when(sums[a])
        def _():
            pl.semaphore_signal(barrier, inc=1, device_id=(h + (1 << a), r, d), device_id_type=MESH)

        @pl.when(gives[a])
        def _():
            pl.semaphore_signal(barrier, inc=1, device_id=(h - (1 << a), r, d), device_id_type=MESH)

    for copy in loads:
        copy.start()
    drain(places, load.at[3])
    for copy in small[3:]:
        copy.wait()
    bins = places[2]
    row_bin = bins // BINS
    down_at = places[0].astype(jnp.float32) + (row_bin.astype(jnp.float32) + 0.5) / BINS
    over_at = places[1].astype(jnp.float32) + ((bins - row_bin * BINS).astype(jnp.float32) + 0.5) / BINS
    for s in range(STEPS):
        spots[0, s, 0:1, :] = down_at[s:s + 1]
        spots[0, s, 1:2, :] = over_at[s:s + 1]
    charges[0] = charge_in[...].astype(jnp.float32).reshape(1, -1)
    pl.semaphore_wait(barrier, count)

    def remote(src, dst, s_sem, r_sem, device):
        return pltpu.make_async_remote_copy(src_ref=src, dst_ref=dst, send_sem=s_sem, recv_sem=r_sem,
                                            device_id=device, device_id_type=MESH)

    def spot_copy(shift, s):
        return remote(spots.at[0, s], spots.at[shift, s], sent.at[0], sem_a.at[s],
                      plane_peer(rows, dom, shift)[1])

    def charge_copy(shift):
        return remote(charges.at[0], charges.at[shift], sent.at[1], once.at[0], plane_peer(rows, dom, shift)[1])

    def tail_copy(s):
        columns = pl.ds(pl.multiple_of(d * width, width), width)
        return remote(old_ref.at[lags - 1 - s, :, columns], gath.at[d, s], sent.at[2], sem_h.at[s], up)

    def tree_copy(s, a):
        return remote(summed.at[s], arrived.at[s, a], sent.at[3], sem_c.at[s, a], (h - (1 << a), r, d))

    def cross_copy(s, j):
        return remote(gath.at[d, s], gath.at[d, s], sent.at[4], sem_x.at[s, j - 1], across[j - 1])

    def partner_copy(s):
        return remote(gath.at[d, s], gath.at[d, s], sent.at[4], sem_g.at[s], partner)

    def forward_copy(s, j):
        other = lax.rem(d + CORES * (chips - j), dom)
        return remote(gath.at[other, s], gath.at[other, s], sent.at[4], sem_g.at[s], partner)

    def span(c):
        return pl.ds(pl.multiple_of(c * size, size), size)

    def row_copy(c, j):
        other = lax.rem(r + j, rows)
        return remote(parts.at[other, span(c)], got.at[j - 1, span(c)], sent.at[5], sem_y.at[c, j - 1],
                      (h, other, d))

    def up_copy(c):
        return remote(to_high.at[span(c)], from_low.at[span(c)], sent.at[6], sem_u.at[c], up)

    def down_copy(c):
        return remote(to_low.at[span(c)], from_high.at[span(c)], sent.at[7], sem_d.at[c], down)

    def kick_copy(k):
        return remote(kicks.at[k], got_kicks.at[k], sent.at[8], once.at[1], plane_peer(rows, dom, n - k)[1])

    def fresh(s):
        return pltpu.make_async_copy(grids.at[STEPS - 1 - s], newest.at[STEPS - 1 - s], load.at[6])

    for s in range(STEPS):
        for shift in range(1, n):
            spot_copy(shift, s).start()
            if s == 0:
                charge_copy(shift).start()

    @pl.when(below)
    def _():
        for s in range(STEPS):
            tail_copy(s).start()

    total[...] = jnp.zeros_like(total)
    dens[...] = jnp.zeros_like(dens)
    kicks[...] = jnp.zeros_like(kicks)
    for copy in loads:
        copy.wait()

    def add_field(weights, mixed, where):
        for comp in range(2):
            total[comp, where] += jnp.dot(mixed, weights[comp], preferred_element_type=jnp.float32)

    def products(k, weights, begin, steps, first=0):
        window = grids[pl.ds(begin, steps)].reshape(steps * band, NG)
        mixed = lax.dot_general(cols[k], window, NT, preferred_element_type=jnp.float32).astype(kind)
        stacked = jnp.concatenate(
            [mixed[:, (steps - 1 - s) * band:(steps - s) * band] for s in range(steps)], axis=0)
        add_field(weights, stacked, pl.ds(first * width, steps * width))

    def whole_lag(k):
        products(k, pltpu.einshape("acb->cab", raw[k]), k, STEPS)

    ahead = max(0, lags - STEPS - 2)

    def lag(k, carry):
        whole_lag(k)
        return carry

    lax.fori_loop(STEPS, STEPS + ahead, lag, 0)
    turned[0] = pltpu.einshape("acb->cab", raw[0])
    for k in range(1, STEPS):
        turned[k] = pltpu.einshape("acb->cab", raw[k])
        products(k, turned[k], STEPS, k)

    side = lax.broadcasted_iota(jnp.int32, (2, 1), 0)
    corner = jnp.where(side == 0, r * band, d * width).astype(jnp.float32)

    def settle(k, s):
        value = spots[k, s]
        floor = jnp.floor(value)
        base[k, s] = floor - corner
        frac[k, s] = value - floor

    def hats(k, s):
        whole, part = base[k, s], frac[k, s]
        left = hat(band, whole[0:1], 1.0 - part[0:1], part[0:1])
        right = hat(width, whole[1:2], 1.0 - part[1:2], part[1:2])
        return left, right

    def deposit(s):
        drain(spots.at[pl.ds(1, n - 1), s], sem_a.at[s])

        @pl.when(s == 0)
        def _():
            drain(charges.at[pl.ds(1, n - 1)], once.at[0])

        def arrive(k, carry):
            settle(k, s)
            return carry

        lax.fori_loop(0, n, arrive, 0, unroll=8)

        def block(k, carry):
            left, right = hats(k, s)
            if keep:
                lefts[k, s] = left
                rights[k, s] = right
            left = left * charges[k].astype(kind)
            dens[s] += lax.dot_general(left, right, NT, preferred_element_type=jnp.float32)
            return carry

        lax.fori_loop(0, n, block, 0, unroll=8)

    def relay(s):
        for a in range(levels):
            @pl.when(sums[a])
            def _():
                tree_copy(s, a).wait_recv()
                dens[s] += arrived[s, a].astype(jnp.float32)

        @pl.when(is_first)
        def _():
            gath[d, s] = dens[s].astype(kind)

        @pl.when(above)
        def _():
            summed[s] = dens[s].astype(kind)

        for a in range(levels):
            @pl.when(gives[a])
            def _():
                tree_copy(s, a).start()

    def gather(s):
        @pl.when(above)
        def _():
            tail_copy(s).wait_recv()

        for j in range(1, chips):
            cross_copy(s, j).start()
        partner_copy(s).start()

    def forward(s):
        for j in range(1, chips):
            cross_copy(s, j).wait_recv()
            forward_copy(s, j).start()

    def assemble(s):
        drain(gath.at[pl.ds(0, chips), s], sem_g.at[s])
        grids[STEPS - 1 - s] = jnp.concatenate([gath[e, s] for e in range(dom)], axis=1)
        fresh(s).start()

    def strip(s):
        return pl.ds(pl.multiple_of(s * width, width), width)

    def post(s):
        where = strip(s)
        for q in range(rows):
            block = jnp.concatenate([total[comp, where, q * piece:(q + 1) * piece] for comp in range(2)], axis=1)

            @pl.when(r == q)
            def _():
                mine[where] = block

            @pl.when(r != q)
            def _():
                parts[q, where] = block.astype(kind)

        for half in range(HALVES):
            for j in range(1, rows):
                row_copy(s * HALVES + half, j).start()

    def add_late(k, s):
        mixed = lax.dot_general(cols[k], grids[STEPS - 1 - s], NT, preferred_element_type=jnp.float32).astype(kind)
        add_field(turned[k], mixed, strip(s + k))

    def late(s):
        assemble(s)
        add_late(0, s)
        post(s)

    def late_more(s):
        def add(k, carry):
            add_late(k, s)
            return carry

        lax.fori_loop(1, STEPS - s, add, 0)

    def late_all(_):
        for s in range(STEPS):
            assemble(s)
        for k in range(STEPS):
            products(k, turned[k], k, STEPS - k, k)
        for s in range(STEPS):
            post(s)

    def spread(c):
        value = mine[span(c)]
        for j in range(1, rows):
            row_copy(c, j).wait_recv()
            value += got[j - 1, span(c)].astype(jnp.float32)
        mine[span(c)] = value

        @pl.when(is_first)
        def _():
            to_high[span(c)] = value.astype(kind)
            up_copy(c).start()

        @pl.when(is_last)
        def _():
            to_low[span(c)] = value.astype(kind)
            down_copy(c).start()

    def rise(c):
        up_copy(c).wait_recv()

        @pl.when(inner)
        def _():
            to_high[span(c)] = (mine[span(c)] + from_low[span(c)].astype(jnp.float32)).astype(kind)
            up_copy(c).start()

    def sink(c):
        down_copy(c).wait_recv()

        @pl.when(inner)
        def _():
            to_low[span(c)] = (mine[span(c)] + from_high[span(c)].astype(jnp.float32)).astype(kind)
            down_copy(c).start()

    def side_hat(k, s, c):
        tall = 2 * size
        whole, part = base[k, s], frac[k, s]
        shift = ((lax.rem(c, HALVES) // 2) * tall).astype(jnp.float32)
        return hat(tall, whole[1:2] - shift, 1.0 - part[1:2], part[1:2]).astype(jnp.float32)

    def kick(c):
        s, part = c // HALVES, lax.rem(c, 2)
        share, tall = n // 2, 2 * size
        rows_c = pl.ds(pl.multiple_of((c // 2) * tall, tall), tall)
        cols_c = pl.ds(pl.multiple_of((lax.rem(c, HALVES) // 2) * tall, tall), tall)

        @pl.when(part == 0)
        def _():
            value = mine[rows_c]
            value += jnp.where(above, from_low[rows_c].astype(jnp.float32), 0.0)
            value += jnp.where(below, from_high[rows_c].astype(jnp.float32), 0.0)
            table[0:tall] = value[:, :band].astype(kind)
            table[tall:] = value[:, band:].astype(kind)

        def block(i, carry):
            k = part * share + i
            left = lefts[k, s] if keep else hats(k, s)[0]
            right = rights[k, s, cols_c].astype(jnp.float32) if keep else side_hat(k, s, c)
            along = jnp.dot(table[...], left, preferred_element_type=jnp.float32)
            for comp in range(2):
                kicks[k, comp:comp + 1, :] += jnp.sum(
                    along[comp * tall:(comp + 1) * tall] * right, axis=0, keepdims=True)
            return carry

        lax.fori_loop(0, share, block, 0, unroll=4)

    early, level, pieces = STEPS + 1, 2 * levels, STEPS * HALVES
    begin, hop = HALVES * (early + 1), HALVES
    zero = HALVES * (level + 3) + HALVES // 2
    zero = HALVES * (level + 3) + 2
    row_lag = jnp.where(is_first, zero, begin)
    rise_lag = begin + 7 + 5 * (h - 1)
    sink_lag = jnp.where(is_first, zero + 11, begin + 4 + 4 * (hist - 2 - h))
    kick_lag = jnp.where(is_first, sink_lag, jnp.where(is_last, rise_lag, jnp.maximum(rise_lag, sink_lag))) + 1
    last = max(zero + 12, begin + 8 + 5 * (hist - 2), begin + max(8 + 5 * (hist - 3), 4 + 4 * (hist - 3))) + 1

    def at(index, action, count=STEPS):
        @pl.when(inside(index, count))
        def _():
            action(index)

    def tick(t, carry):
        at(t, deposit)

        @pl.when(is_first)
        def _():
            at(t - level - 2, late)

        at(t - 2 * rank, relay)
        at(jnp.where(is_first, t - level, 2 * t), gather)

        @pl.when(above)
        def _():
            at(2 * t + 1, gather)
            at(t - early, late_all, 1)

        def turn(i, carry):
            c = HALVES * t + i
            at(c - row_lag, spread, pieces)

            @pl.when(jnp.logical_and(below, sink_first))
            def _():
                at(c - sink_lag, sink, pieces)

            @pl.when(above)
            def _():
                at(c - rise_lag, rise, pieces)

            @pl.when(jnp.logical_not(sink_first))
            def _():
                at(c - sink_lag, sink, pieces)

            at(c - kick_lag, kick, pieces)
            return carry

        @pl.when(t >= min(early + 1, level + 3))
        def _():
            lax.fori_loop(0, HALVES, turn, 0)

        at(jnp.where(is_first, t - level - 1, 2 * (t - STEPS + 1)), forward)

        @pl.when(above)
        def _():
            at(2 * (t - STEPS + 1) + 1, forward)

        @pl.when(is_first)
        def _():
            at(t - level - 2, late_more)

        spare = STEPS + ahead + jnp.where(is_first, t - STEPS, t - STEPS + 1)

        @pl.when(jnp.logical_and(spare >= STEPS + ahead, spare < lags))
        def _():
            whole_lag(spare)

        return carry

    sink_first = h > 0
    lax.fori_loop(0, -(-(last + pieces) // HALVES), tick, 0)

    for k in range(1, n):
        kick_copy(k).start()
    drain(spots.at[pl.ds(0, n - 1)], sent.at[0])
    drain(charges.at[pl.ds(0, n - 1)], sent.at[1])
    drain(gath.at[pl.ds(0, 2 * chips - 1)], sent.at[4])
    drain(got, sent.at[5])
    pltpu.make_async_copy(grids.at[pl.ds(0, STEPS)], newest, load.at[6]).wait()

    @pl.when(above)
    def _():
        drain(summed, sent.at[3])
        drain(from_high, sent.at[7])

    @pl.when(below)
    def _():
        drain(gath.at[0], sent.at[2])
        drain(from_low, sent.at[6])

    drain(kicks.at[pl.ds(0, n - 1)], sent.at[8])
    drain(got_kicks.at[pl.ds(1, n - 1)], once.at[1])
    sum_all = kicks[0]
    for k in range(1, n):
        sum_all = sum_all + got_kicks[k]
    out[...] = start[...] + kick_scale * sum_all


def finish_kernel(moved, newest, old, out, history, writes):
    fresh, kept = newest.shape[0], history.shape[0] - newest.shape[0]
    stores = (pltpu.make_async_copy(newest, history.at[pl.ds(0, fresh)], writes.at[0]),
              pltpu.make_async_copy(old.at[pl.ds(0, kept)], history.at[pl.ds(fresh, kept)], writes.at[1]),
              pltpu.make_async_copy(moved, out, writes.at[2]))
    for copy in stores:
        copy.start()
    for copy in stores:
        copy.wait()


def finish(moved, newest, history):
    anywhere = pl.BlockSpec(memory_space=pl.ANY)
    return pl.pallas_call(
        finish_kernel,
        out_shape=(jax.ShapeDtypeStruct(moved.shape, moved.dtype), jax.ShapeDtypeStruct(history.shape, history.dtype)),
        in_specs=[VM] * 3, out_specs=(anywhere, anywhere),
        scratch_shapes=[pltpu.SemaphoreType.DMA((3,))],
        compiler_params=pltpu.CompilerParams(vmem_limit_bytes=8 * 2 ** 20),
    )(moved, newest, history)


def local(hist, rows, dom, row_index, col_index, bin_index, charge, momentum, history, kernel_cols, kernel_rows):
    lags, band, _ = history.shape
    width = kernel_cols.shape[1]
    own = row_index.shape[1]
    n = rows * dom
    chips, levels = dom // CORES, (hist - 1).bit_length()
    tall, wide = STEPS * width, 2 * NG // rows
    count = STEPS * HALVES
    kind, wider = jnp.bfloat16, jnp.float32
    dma, vmem = pltpu.SemaphoreType.DMA, pltpu.VMEM
    anywhere = pl.BlockSpec(memory_space=pl.ANY)
    tile = (STEPS, band, width)
    flat = vmem((tall, wide), kind)
    each = vmem((n,) + momentum.shape, wider)
    kept = n if n * STEPS * (band + width) * own * 2 <= 32 * 2 ** 20 else 1
    steps = (STEPS, own)
    spot = vmem((n, STEPS, 2, own), wider)
    moved, newest = pl.pallas_call(
        functools.partial(kernel, hist, rows, dom),
        out_shape=(jax.ShapeDtypeStruct(momentum.shape, wider),
                   jax.ShapeDtypeStruct((STEPS, band, NG), kind)),
        in_specs=[pl.BlockSpec(memory_space=pltpu.HBM)] * 8, out_specs=(VM, anywhere),
        scratch_shapes=[vmem((3,) + steps, jnp.int32), vmem((own,), kind),
                        vmem(momentum.shape, wider), spot, vmem((n, 1, own), wider), spot, spot,
                        vmem((kept, STEPS, band, own), kind), vmem((kept, STEPS, width, own), kind),
                        vmem(tile, wider), vmem(tile, kind), vmem((STEPS, levels) + tile[1:], kind),
                        vmem((dom,) + tile, kind), vmem((lags + STEPS, band, NG), kind),
                        vmem(kernel_cols.shape, kind), vmem(kernel_rows.shape, kind),
                        vmem((STEPS, 2, band, NG), kind), vmem((2, tall, NG), wider),
                        vmem((rows, tall, wide), kind), vmem((rows - 1, tall, wide), kind), vmem((tall, wide), wider),
                        flat, flat, flat, flat, vmem((4 * width // HALVES, band), kind), each, each, dma((7,)), dma((9,)), dma((2,)), dma((STEPS,)),
                        dma((STEPS,)), dma((STEPS, levels)), dma((STEPS, chips - 1)), dma((STEPS,)),
                        dma((count, rows - 1)), dma((count,)), dma((count,))],
        compiler_params=pltpu.CompilerParams(collective_id=1, has_side_effects=True,
                                             vmem_limit_bytes=50 * 2 ** 20),
    )(*(pltpu.with_memory_space_constraint(x, pltpu.HBM) for x in (
        row_index, col_index, bin_index, charge, momentum, history, kernel_cols, kernel_rows)))
    return finish(moved, newest, history)


def solution(mesh):
    spread = ("hist", "rows", "dom")
    in_specs = (P(None, spread), P(None, spread), P(None, spread), P(spread), P(None, spread),
                P("hist", "rows", None), P("hist", "dom", None), P("hist", "rows", None, None))
    out_specs = (P(None, spread), P("hist", "rows", None))
    sizes = mesh.shape
    body = functools.partial(local, sizes["hist"], sizes["rows"], sizes["dom"])
    return jax.shard_map(body, mesh=mesh, in_specs=in_specs, out_specs=out_specs, check_vma=False)
```
